32 devices in a mesh: replica: 4 (over z), shard: 8 (over y, x, core).
Axes of the slice: x: 2, y: 2, z: 4, core: 2. Of those that a mesh axis runs over, the one named last changes fastest.
Arguments:
- observations: bfloat16 [2048, 16, 1024], P(('replica', 'shard')), may hold values from -6 to 6
- rewards: float32 [2048, 16], P(('replica', 'shard')), may hold values from -6 to 6
- actions: int32 [2048, 21], P(('replica', 'shard')), may hold values from 0 to 17
- lengths: int32 [2048], P(('replica', 'shard')), may hold values from 1 to 16
- nsteps: int32 [2048], P(('replica', 'shard')), may hold values from 1 to 10
- prio_index: int32 [2048, 4], P(('replica', 'shard')), may hold values from 0 to 15
- assignment: int32 [2048, 1], P(('replica', 'shard')), may hold values from 0 to 3; in each aligned block of 64 rows (0 to 63, 64 to 127, ...) at most 32 rows name the same one
- rep_weight: bfloat16 [4, 1024, 512], P('replica', 'shard'), may hold values from -0.1875 to 0.1875
- dyn_in: bfloat16 [4, 512, 512], P('replica', 'shard'), may hold values from -0.25 to 0.25
- dyn_out: bfloat16 [4, 512, 512], P('replica', 'shard'), may hold values from -0.25 to 0.25
- value_hidden: bfloat16 [4, 512, 512], P('replica', 'shard'), may hold values from -0.25 to 0.25
- action_table: bfloat16 [4, 18, 512], P('replica'), may hold values from -6 to 6
- value_out: bfloat16 [4, 512], P('replica'), may hold values from -0.25 to 0.25
- reward_out: bfloat16 [4, 512], P('replica'), may hold values from -0.25 to 0.25
Outputs:
- priorities: float32 [2048, 4], P(('replica', 'shard'))
The draws below stay inside these ranges and needn't reach their ends.
Inputs may be any that keep to these rules, and one draw needn't show every extreme that they name: `assignment`: among the 64 trajectories of one device (aligned blocks), at most 32 name one group; in some block one group is named by exactly 32.
All inputs are finite; a program needn't handle non-finite values.
Results may differ from the reference program's by a relative error of at most 0.0065.
Values may be sent and summed in bfloat16 or wider, within the bound.
A program may use at most 128 MiB of HBM per device.

```python
import math
import jax
import jax.numpy as jnp
import numpy as np
from jax import lax

F = 1024
H = 512
ACTIONS = 18
STEPS = 16
UNROLL = 5
NMAX = 10
PRIO = 4
TRAJ_DEV = 64
MOSTG = 32
GROUPS = 4
TRAJECTORIES = 2048


def plant(drawn, rng, least, largest):
    dims = drawn.shape
    place = [jax.random.randint(jax.random.fold_in(rng, axis), (), 0, dims[axis]) for axis in range(len(dims))]
    drawn = drawn.at[tuple(place)].set(least)
    longest = dims.index(max(dims))
    place[longest] = (place[longest] + 1) % dims[longest]
    return drawn.at[tuple(place)].set(largest)


def block_scale(own_key, extent, pieces, smallest, largest):
    gain, own = 1.0, jax.random.fold_in(own_key, 6)
    for dim, shards_of in pieces:
        steps = jnp.exp(jax.random.uniform(jax.random.fold_in(own, dim), (shards_of,), jnp.float32, smallest / len(pieces), largest / len(pieces)))
        gain = gain * jnp.repeat(steps, extent[dim] // shards_of).reshape([-1 if axis == dim else 1 for axis in range(len(extent))])
    return gain


def shared_out(key, own, number, rows, amount, top, limit, lean):
    sequence = jax.random.permutation(key, amount)
    heavy_load, usual = load_shares(amount, rows * top, limit, lean, True), load_shares(amount, rows * top, limit, lean, False)
    places = jnp.arange(amount)

    def named(sizes, rotation):
        used = int((sizes > 0).sum())
        fixed = max(1, used // 4)
        passed = fixed + (places - fixed + rotation * (used - fixed)) % max(1, amount - fixed)
        return jnp.zeros((amount,), jnp.int32).at[sequence[jnp.where(places < fixed, places, passed)]].set(jnp.asarray(sizes, jnp.int32))

    sizes = jnp.where(number % 4 == 0, named(heavy_load, number // 4), named(usual, number - number // 4 - 1))
    mixed = jax.random.permutation(jax.random.fold_in(own, 3), amount)
    giver, receiver = mixed[0:amount // 2 * 2:2], mixed[1:amount // 2 * 2:2]
    margin = jnp.minimum(sizes[giver] - 1, limit - sizes[receiver]) // 2
    margin = jnp.where((giver == sequence[0]) | (receiver == sequence[0]) | (sizes[receiver] == 0), 0, jnp.maximum(margin, 0))
    passed = jax.random.randint(jax.random.fold_in(own, 4), (amount // 2,), 0, 1 << 20) % (margin + 1)
    sizes = sizes.at[giver].add(-passed).at[receiver].add(passed)
    items = jnp.searchsorted(jnp.cumsum(sizes), jnp.arange(rows * top), side="right").astype(jnp.int32)
    table = items.reshape(top, rows).T
    table = table[jax.random.permutation(jax.random.fold_in(own, 1), rows)]
    rotation = jax.random.randint(jax.random.fold_in(own, 2), (rows, 1), 0, top)
    return jnp.take_along_axis(table, (jnp.arange(top)[None, :] + rotation) % top, axis=1)


def load_shares(count, total, most, lean, full):
    weights = [(1 << 20) // math.isqrt(grade ** lean) + 1 for grade in range(1, count + 1)]
    largest = most if full else min(most, max(-(-total // count), total * weights[0] // sum(weights)))
    least = 1 if total - largest >= count - 1 else 0
    counts, rest = [largest] + [least] * (count - 1), total - largest - least * (count - 1)
    while rest > 0:
        candidates = [i for i in range(1, count) if counts[i] < largest] or [i for i in range(1, count) if counts[i] < most]
        whole, remaining = sum([weights[i] for i in candidates]), rest
        for i in candidates:
            more = min(most - counts[i], max(1, remaining * weights[i] // whole), rest)
            counts[i] = counts[i] + more
            rest = rest - more
    return np.array(counts)


def noise(own_key, dims, spread, limit, cuts=(), kind=jnp.bfloat16):
    values = jax.random.normal(own_key, dims, jnp.float32) * spread
    if len(cuts) > 0:
        values = block_scale(own_key, dims, cuts, -0.22, 0.18) * values
    return jnp.clip(values, min=-limit, max=limit).astype(kind)


def setup_inputs(seed: int = 0) -> dict:
    streams_of = jax.random.split(jax.random.key(seed), 15)
    observations = noise(streams_of[0], (TRAJECTORIES, STEPS, F), 1.0, 6.0, ((0, 32),))
    rewards = noise(streams_of[1], (TRAJECTORIES, STEPS), 1.0, 6.0, ((0, 32),), jnp.float32)
    actions = plant(jax.random.randint(streams_of[2], (TRAJECTORIES, STEPS + UNROLL), 0, ACTIONS), jax.random.fold_in(streams_of[2], 1), 0, ACTIONS - 1).astype(jnp.int32)
    lengths = plant(jax.random.randint(streams_of[3], (TRAJECTORIES,), 1, STEPS + 1), jax.random.fold_in(streams_of[3], 1), 1, STEPS).astype(jnp.int32)
    nsteps = plant(jax.random.randint(streams_of[4], (TRAJECTORIES,), 1, NMAX + 1), jax.random.fold_in(streams_of[4], 1), 1, NMAX).astype(jnp.int32)
    prio_index = plant(jax.random.randint(streams_of[5], (TRAJECTORIES, PRIO), 0, STEPS), jax.random.fold_in(streams_of[5], 1), 0, STEPS - 1).astype(jnp.int32)
    assignment_keys = jax.random.split(jax.random.fold_in(streams_of[6], 1), TRAJECTORIES // TRAJ_DEV)
    assignment_turns = jax.random.permutation(jax.random.fold_in(streams_of[6], 3), TRAJECTORIES // TRAJ_DEV)
    assignment = jax.vmap(lambda own, number: shared_out(jax.random.fold_in(streams_of[6], 2), own, number, TRAJ_DEV, GROUPS, 1, MOSTG, 2))(assignment_keys, assignment_turns).reshape((TRAJECTORIES, 1))
    rep_weight = noise(streams_of[7], (GROUPS, F, H), F ** -0.5, 0.1875, ((0, 4), (1, 8)))
    dyn_in = noise(streams_of[8], (GROUPS, H, H), H ** -0.5, 0.25, ((0, 4), (1, 8)))
    dyn_out = noise(streams_of[9], (GROUPS, H, H), H ** -0.5, 0.25, ((0, 4), (1, 8)))
    value_hidden = noise(streams_of[10], (GROUPS, H, H), H ** -0.5, 0.25, ((0, 4), (1, 8)))
    action_table = noise(streams_of[11], (GROUPS, ACTIONS, H), 1.0, 6.0, ((0, 4),))
    value_out = noise(streams_of[12], (GROUPS, H), H ** -0.5, 0.25, ((0, 4),))
    reward_out = noise(streams_of[13], (GROUPS, H), H ** -0.5, 0.25, ((0, 4),))
    return {"observations": observations, "rewards": rewards, "actions": actions, "lengths": lengths, "nsteps": nsteps, "prio_index": prio_index, "assignment": assignment, "rep_weight": rep_weight, "dyn_in": dyn_in, "dyn_out": dyn_out, "value_hidden": value_hidden, "action_table": action_table, "value_out": value_out, "reward_out": reward_out}


discount = 0.997
epsilon = 1e-06

def rms_scale(values):
    return values * lax.rsqrt(lax.optimization_barrier(jnp.mean(values * values, axis=-1, keepdims=True)) + epsilon)

def value_head(latent, hidden_weight, value_vector):
    inner = jnp.maximum(jnp.dot(latent, hidden_weight, preferred_element_type=jnp.float32), 0.0).astype(jnp.bfloat16)
    return jnp.dot(inner, value_vector, preferred_element_type=jnp.float32)

def evaluate(frames, rewards, moves, lengths, nsteps, picks, network):
    rep_weight, dyn_in, dyn_out, value_hidden, action_table, value_out, reward_out = network
    batch, steps, width = frames.shape
    unroll = moves.shape[1] - steps
    flat = frames.reshape(batch * steps, width)
    latent = rms_scale(jnp.dot(flat, rep_weight, preferred_element_type=jnp.float32)).astype(jnp.bfloat16)
    root_value = value_head(latent, value_hidden, value_out).reshape(batch, steps)
    action_count = action_table.shape[0]
    model_return = jnp.zeros((batch * steps,), jnp.float32)
    state = latent
    for depth in range(unroll):
        chosen = moves[:, depth:depth + steps].reshape(batch * steps)
        one_hot = (chosen[:, None] == jnp.arange(action_count, dtype=jnp.int32)[None, :]).astype(jnp.bfloat16)
        embedded = jnp.dot(one_hot, action_table, preferred_element_type=jnp.float32)
        inner = jnp.maximum(jnp.dot(state, dyn_in, preferred_element_type=jnp.float32) + embedded, 0.0).astype(jnp.bfloat16)
        update = jnp.dot(inner, dyn_out, preferred_element_type=jnp.float32)
        state = rms_scale(state.astype(jnp.float32) + update).astype(jnp.bfloat16)
        reward_guess = jnp.dot(state, reward_out, preferred_element_type=jnp.float32)
        model_return = model_return + discount ** depth * reward_guess
    model_return = model_return + discount ** unroll * value_head(state, value_hidden, value_out)
    model_return = model_return.reshape(batch, steps)
    position = jnp.arange(steps, dtype=jnp.int32)
    offset = position[None, :] - position[:, None]
    live = position[None, :] < lengths[:, None]
    horizon = nsteps[:, None, None]
    inside = (offset[None] >= 0) & (offset[None] < horizon) & live[:, None, :]
    power = discount ** jnp.maximum(offset, 0).astype(jnp.float32)
    weights = jnp.where(inside, power[None], 0.0)
    boot = (offset[None] == horizon) & live[:, None, :]
    boot_weights = jnp.where(boot, discount ** horizon.astype(jnp.float32), 0.0)
    target = lax.optimization_barrier(jnp.sum(weights * rewards[:, None, :] + boot_weights * model_return[:, None, :], axis=2))
    priority = jnp.abs(target - root_value)
    pick = picks[:, :, None] == position[None, None, :]
    return lax.optimization_barrier(jnp.sum(jnp.where(pick, priority[:, None, :], 0.0), axis=2))

def ranks_within(owner, groups):
    member = (owner[:, None] == jnp.arange(groups, dtype=jnp.int32)[None, :]).astype(jnp.int32)
    earlier = jnp.cumsum(member, axis=0) - member
    return lax.optimization_barrier(jnp.sum(earlier * member, axis=1))

def reference(observations, rewards, actions, lengths, nsteps, prio_index, assignment, rep_weight, dyn_in, dyn_out, value_hidden, action_table, value_out, reward_out):
    groups = rep_weight.shape[0]
    blocks = observations.shape[0] // TRAJ_DEV

    def one_block(index):
        start = (index * TRAJ_DEV).astype(jnp.int32)

        def take(array):
            return lax.dynamic_slice_in_dim(array, start, TRAJ_DEV, 0)
        frames = take(observations)
        reward_rows = take(rewards)
        moves = take(actions)
        length_rows = take(lengths)
        step_rows = take(nsteps)
        picks = take(prio_index)
        owner = take(assignment)[:, 0]
        rank = ranks_within(owner, groups)
        result = jnp.zeros((TRAJ_DEV, PRIO), jnp.float32)
        for group in range(groups):
            spot = jnp.where(owner == group, rank, MOSTG)
            match = spot[None, :] == jnp.arange(MOSTG, dtype=jnp.int32)[:, None]
            source = lax.optimization_barrier(jnp.sum(jnp.where(match, jnp.arange(TRAJ_DEV, dtype=jnp.int32)[None, :], 0), axis=1)).astype(jnp.int32)
            network = (rep_weight[group], dyn_in[group], dyn_out[group], value_hidden[group], action_table[group], value_out[group], reward_out[group])
            picked = evaluate(frames[source], reward_rows[source], moves[source], length_rows[source], step_rows[source], picks[source], network)
            back = jnp.take(picked, jnp.minimum(spot, MOSTG - 1), axis=0)
            result = jnp.where((owner == group)[:, None], back, result)
        return result
    output = lax.map(one_block, jnp.arange(blocks, dtype=jnp.int32))
    return output.reshape(blocks * TRAJ_DEV, PRIO)
```

```python
import jax
import jax.numpy as jnp
from jax import lax
from jax.sharding import PartitionSpec as P

MOSTG = 32


discount = 0.997
epsilon = 1e-06


def rms_scale(values):
    return values * lax.rsqrt(jnp.mean(values * values, axis=-1, keepdims=True) + epsilon)


def matmul(rows, weights):
    return jnp.einsum("gmk,gkn->gmn", rows, weights, preferred_element_type=jnp.float32)


def ranks_within(owner, groups):
    member = (owner[:, None] == jnp.arange(groups, dtype=jnp.int32)[None, :]).astype(jnp.int32)
    earlier = jnp.cumsum(member, axis=0) - member
    return jnp.sum(earlier * member, axis=1)


def reward_part(rewards, lengths, nsteps, picks):
    position = jnp.arange(rewards.shape[1], dtype=jnp.int32)
    offset = position[None, None, :] - picks[:, :, None]
    inside = (
        (offset >= 0)
        & (offset < nsteps[:, None, None])
        & (position[None, None, :] < lengths[:, None, None])
    )
    power = discount ** jnp.maximum(offset, 0).astype(jnp.float32)
    return jnp.sum(jnp.where(inside, power, 0.0) * rewards[:, None, :], axis=2)


def on_device(
    observations,
    rewards,
    actions,
    lengths,
    nsteps,
    prio_index,
    assignment,
    rep_weight,
    dyn_in,
    dyn_out,
    value_hidden,
    action_table,
    value_out,
    reward_out,
):
    groups = lax.axis_size("replica")
    batch, steps, width = observations.shape
    unroll = actions.shape[1] - steps
    picks = prio_index.shape[1]
    both = ("replica", "shard")

    def whole(weight):
        part = lax.all_gather(weight, both, axis=0, tiled=True)
        return part.reshape(groups, -1, weight.shape[-1])

    full_rep, full_in, full_out, full_value = (
        whole(rep_weight),
        whole(dyn_in),
        whole(dyn_out),
        whole(value_hidden),
    )
    small = jnp.concatenate([action_table[0], value_out, reward_out], axis=0)
    small = lax.all_gather(small, "replica", axis=0)
    action_count = action_table.shape[1]
    tables = small[:, :action_count]
    value_vector = small[:, action_count]
    reward_vector = small[:, action_count + 1]

    owner = assignment[:, 0]
    spot = owner * MOSTG + ranks_within(owner, groups)
    slots = groups * MOSTG
    match = spot[None, :] == jnp.arange(slots, dtype=jnp.int32)[:, None]
    source = jnp.sum(
        jnp.where(match, jnp.arange(batch, dtype=jnp.int32)[None, :], 0), axis=1
    )
    reach = prio_index + nsteps[:, None]
    alive = reach < lengths[:, None]
    reach = jnp.minimum(reach, steps - 1)
    base = jnp.arange(batch, dtype=jnp.int32)[:, None] * steps
    rows = jnp.concatenate([base + prio_index, base + reach], axis=1)
    moves = jnp.concatenate(
        [jnp.take_along_axis(actions, reach + depth, axis=1) for depth in range(unroll)], axis=1
    )
    packed = jnp.take(jnp.concatenate([rows, moves], axis=1), source, axis=0)
    packed = packed.reshape(groups, MOSTG, (2 + unroll), picks).transpose(0, 2, 1, 3)
    packed = packed.reshape(groups, 2 + unroll, MOSTG * picks)
    lines = packed[:, :2].reshape(-1)
    frames = jnp.take(observations.reshape(batch * steps, width), lines, axis=0)
    frames = frames.reshape(groups, 2 * MOSTG * picks, width)

    latent = rms_scale(matmul(frames, full_rep)).astype(jnp.bfloat16)
    state = latent[:, MOSTG * picks :]
    model_return = 0.0
    for depth in range(unroll):
        chosen = packed[:, 2 + depth]
        one_hot = (
            chosen[:, :, None] == jnp.arange(action_count, dtype=jnp.int32)[None, None, :]
        ).astype(jnp.bfloat16)
        inner = jnp.maximum(matmul(state, full_in) + matmul(one_hot, tables), 0.0).astype(
            jnp.bfloat16
        )
        state = rms_scale(state.astype(jnp.float32) + matmul(inner, full_out)).astype(
            jnp.bfloat16
        )
        guess = jnp.einsum(
            "gmk,gk->gm", state, reward_vector, preferred_element_type=jnp.float32
        )
        model_return = model_return + discount**depth * guess
    ends = jnp.concatenate([latent[:, : MOSTG * picks], state], axis=1)
    hidden = jnp.maximum(matmul(ends, full_value), 0.0).astype(jnp.bfloat16)
    values = jnp.einsum(
        "gmk,gk->gm", hidden, value_vector, preferred_element_type=jnp.float32
    )
    root_value = values[:, : MOSTG * picks].reshape(slots, picks)
    model_return = model_return + discount**unroll * values[:, MOSTG * picks :]
    model_return = model_return.reshape(slots, picks)
    back = jnp.take(jnp.concatenate([root_value, model_return], axis=1), spot, axis=0)
    bonus = discount ** nsteps.astype(jnp.float32)
    target = reward_part(rewards, lengths, nsteps, prio_index) + jnp.where(
        alive, bonus[:, None] * back[:, picks:], 0.0
    )
    return jnp.abs(target - back[:, :picks])


def solution(mesh):
    placed = (
        P(("replica", "shard"), None, None),
        P(("replica", "shard"), None),
        P(("replica", "shard"), None),
        P(("replica", "shard")),
        P(("replica", "shard")),
        P(("replica", "shard"), None),
        P(("replica", "shard"), None),
        P("replica", "shard", None),
        P("replica", "shard", None),
        P("replica", "shard", None),
        P("replica", "shard", None),
        P("replica", None, None),
        P("replica", None),
        P("replica", None),
    )
    return jax.shard_map(
        on_device,
        mesh=mesh,
        in_specs=placed,
        out_specs=P(("replica", "shard"), None),
        check_vma=False,
    )
```

```python
import functools
import math

import jax
import jax.numpy as jnp
from jax import lax
from jax.experimental import pallas as pl
from jax.experimental.pallas import tpu as pltpu
from jax.sharding import PartitionSpec as P

MOSTG = 32
CORES = 2
MESH = pl.DeviceIdType.MESH


discount = 0.997
epsilon = 1e-06


def rms_scale(values):
    return values * lax.rsqrt(jnp.mean(values * values, axis=-1, keepdims=True) + epsilon)


def ranks_within(owner, groups):
    member = (owner[:, None] == jnp.arange(groups, dtype=jnp.int32)[None, :]).astype(jnp.int32)
    earlier = jnp.cumsum(member, axis=0) - member
    return jnp.sum(earlier * member, axis=1)


def reward_part(rewards, lengths, nsteps, picks):
    position = jnp.arange(rewards.shape[1], dtype=jnp.int32)
    offset = position[None, None, :] - picks[:, :, None]
    inside = (
        (offset >= 0)
        & (offset < nsteps[:, None, None])
        & (position[None, None, :] < lengths[:, None, None])
    )
    power = discount ** jnp.maximum(offset, 0).astype(jnp.float32)
    return jnp.sum(jnp.where(inside, power, 0.0) * rewards[:, None, :], axis=2)


def chip_cycle(chips):
    side = max(d for d in range(1, math.isqrt(chips) + 1) if chips % d == 0)
    wide = chips // side
    if side % 2 or wide < 2:
        return list(range(chips))
    order = [0]
    for row in range(side):
        columns = range(1, wide) if row % 2 == 0 else range(wide - 1, 0, -1)
        order += [row * wide + column for column in columns]
    return order + [row * wide for row in range(side - 1, 0, -1)]


def lookup(table, index):
    found = jnp.int32(table[0])
    for place in range(1, len(table)):
        found = jnp.where(index == place, jnp.int32(table[place]), found)
    return found


class Copies:
    def __init__(self, send, recv):
        self.send, self.recv, self.made = send, recv, []

    def start(self, source, target, device):
        k = len(self.made)
        copy = pltpu.make_async_remote_copy(
            src_ref=source,
            dst_ref=target,
            send_sem=self.send.at[k],
            recv_sem=self.recv.at[k],
            device_id=device,
            device_id_type=MESH,
        )
        copy.start()
        self.made.append(copy)
        return copy


def network_kernel(
    groups,
    shards,
    unroll,
    action_count,
    obs_ref,
    lines_ref,
    moves_ref,
    rep_ref,
    dyn_ref,
    val_ref,
    small_ref,
    out_ref,
    rep,
    dyn,
    val,
    small,
    latent,
    frames,
    total,
    send,
    recv,
    local,
):
    chips = shards // CORES
    half_ring, half_line = chips // 2, groups // 2
    me = lax.axis_index("replica")
    mine = lax.axis_index("shard")
    chip, core = mine // CORES, mine % CORES
    order = chip_cycle(chips)
    place = lookup([order.index(k) for k in range(chips)], chip)

    def at(distance):
        return lookup(order, lax.rem(place + distance + chips, chips))

    after, before = at(1), at(-1)
    up = (lax.rem(me + 1, groups), mine)
    down = (lax.rem(me + groups - 1, groups), mine)
    right = (me, after * CORES + core)
    left = (me, before * CORES + core)
    sibling = (me, chip * CORES + (1 - core))

    barrier = pltpu.get_barrier_semaphore()
    for device in (up, down, right, left, sibling):
        pl.semaphore_signal(barrier, inc=1, device_id=device, device_id_type=MESH)
    pl.semaphore_wait(barrier, 5)

    copies = Copies(send, recv)
    wide = rep_ref.shape[-1]
    halves = (pl.ds(0, wide // 2), pl.ds(wide // 2, wide // 2))

    def levels():
        return [(0, 1)] + [(2 * d - 1, 2) for d in range(1, half_line)] + [(groups - 1, 1)]

    def line(buffer, own, view, distance):
        pair = []
        for way, device in ((0, up), (1, down)):
            if distance == 1:
                source = own
            else:
                source = view(buffer.at[2 * (distance - 1) - 1 + way])
            last = distance == half_line
            slot = groups - 1 if last else 2 * distance - 1 + way
            target = view(buffer.at[slot])
            if last:
                source = source.at[(slice(None),) * (len(source.shape) - 1) + (halves[way],)]
                target = target.at[(slice(None),) * (len(target.shape) - 1) + (halves[way],)]
            pair.append(copies.start(source, target, device))
        return pair

    def ring(buffer, own, level, distance):
        first, count = level
        pair = []
        for way, device in ((0, right), (1, left)):
            origin = at((1 - distance) if way == 0 else (distance - 1))
            target = buffer.at[pl.ds(first, count), origin, core]
            source = own if own is not None and distance == 1 else target
            if own is not None and distance == 1:
                target = buffer.at[first, origin, core]
            if distance == half_ring:
                source = source.at[(slice(None),) * (len(source.shape) - 1) + (halves[way],)]
                target = target.at[(slice(None),) * (len(target.shape) - 1) + (halves[way],)]
            pair.append(copies.start(source, target, device))
        return pair

    def arrived(pair):
        for copy in pair:
            copy.wait_recv()

    def finish_ring(buffer, level, pair):
        for distance in range(2, half_ring + 1):
            arrived(pair)
            pair = ring(buffer, None, level, distance)
        return pair

    def share(buffer, level):
        first, count = level
        piece = buffer.at[pl.ds(first, count), :, core]
        return copies.start(piece, piece, sibling)

    def block(ref):
        return ref.at[chip, core]

    def plane(ref):
        return ref.at[:, core]

    def whole(ref):
        return ref

    own = []
    for k, (ref, buffer) in enumerate(((rep_ref, rep), (dyn_ref, dyn), (val_ref, val))):
        own.append(pltpu.make_async_copy(ref, buffer.at[0, chip, core], local.at[k]))
    own.append(pltpu.make_async_copy(small_ref, small.at[0], local.at[3]))
    for copy in own:
        copy.start()

    near, far = levels()[0], levels()[1:]
    rep_line = line(rep, rep_ref, block, 1)
    rep_ring = ring(rep, rep_ref, near, 1)
    small_line = line(small, small_ref, whole, 1)
    dyn_line = line(dyn, dyn_ref, block, 1)
    val_ring = ring(val, val_ref, near, 1)
    dyn_ring = ring(dyn, dyn_ref, near, 1)

    rows = lines_ref.shape[1]
    half = rows // 2
    observed = obs_ref.shape[0]

    def pick(slot, carry):
        one_hot = (
            lines_ref[slot] == lax.broadcasted_iota(jnp.int32, (rows, observed), 1)
        ).astype(jnp.bfloat16)
        frames[slot] = jnp.dot(
            one_hot, obs_ref[...], preferred_element_type=jnp.float32
        ).astype(jnp.bfloat16)
        return carry

    lax.fori_loop(0, groups, pick, 0)
    for copy in own:
        copy.wait()

    rep_far, dyn_far = [], []
    for index, level in enumerate(far):
        distance = index + 1
        arrived(rep_line)
        if distance < half_line:
            rep_line = line(rep, None, block, distance + 1)
        rep_far.append(ring(rep, None, level, 1))
        if index == 0:
            rep_ring = finish_ring(rep, near, rep_ring)
            val_ring = finish_ring(val, near, val_ring)
        arrived(small_line)
        if distance < half_line:
            small_line = line(small, None, whole, distance + 1)
        arrived(dyn_line)
        if distance < half_line:
            dyn_line = line(dyn, None, block, distance + 1)
        if index == 0:
            arrived(val_ring)
            val_line = line(val, val.at[0, :, core], plane, 1)
            dyn_ring = finish_ring(dyn, near, dyn_ring)
        dyn_far.append(ring(dyn, None, level, 1))
    shared = []
    for index, level in enumerate(far):
        rep_far[index] = finish_ring(rep, level, rep_far[index])
    arrived(rep_ring)
    rep_shared = [share(rep, near)]
    for index, level in enumerate(far):
        dyn_far[index] = finish_ring(dyn, level, dyn_far[index])
        arrived(rep_far[index])
        rep_shared.append(share(rep, level))
    arrived(dyn_ring)
    dyn_shared = [share(dyn, near)]
    val_shared = [share(val, near)]
    for distance in range(2, half_line + 1):
        arrived(val_line)
        val_line = line(val, None, plane, distance)
        val_shared.append(share(val, far[distance - 2]))
    arrived(rep_shared)

    def represent(slot, carry):
        weight = rep[slot].reshape(-1, wide)
        raw = jnp.dot(frames[slot], weight, preferred_element_type=jnp.float32)
        latent[slot] = rms_scale(raw).astype(jnp.bfloat16)
        return carry

    lax.fori_loop(0, groups, represent, 0)
    for index, level in enumerate(far):
        arrived(dyn_far[index])
        dyn_shared.append(share(dyn, level))
    arrived(dyn_shared)

    rows_in = dyn.shape[3] // 2
    total[...] = jnp.zeros_like(total)

    def advance(depth, scale):
        for slot in range(groups):
            first = dyn[slot, :, :, :rows_in].reshape(-1, wide)
            second = dyn[slot, :, :, rows_in:].reshape(-1, wide)
            table = small[slot]
            one_hot = (
                moves_ref[depth, slot]
                == lax.broadcasted_iota(jnp.int32, (half, table.shape[0]), 1)
            ).astype(jnp.bfloat16)
            state = latent[slot, half:]
            inner = jnp.maximum(
                jnp.dot(state, first, preferred_element_type=jnp.float32)
                + jnp.dot(one_hot, table, preferred_element_type=jnp.float32),
                0.0,
            ).astype(jnp.bfloat16)
            update = jnp.dot(inner, second, preferred_element_type=jnp.float32)
            state = rms_scale(state.astype(jnp.float32) + update).astype(jnp.bfloat16)
            latent[slot, half:] = state
            vector = table.astype(jnp.float32)[action_count + 1 : action_count + 2]
            guess = jnp.sum(state.astype(jnp.float32) * vector, axis=-1, keepdims=True)
            total[slot] = total[slot] + scale * guess
        return scale * discount

    lax.fori_loop(0, unroll, advance, jnp.float32(1.0))
    arrived(val_line)
    val_shared.append(share(val, far[-1]))
    arrived(val_shared)

    for slot in range(groups):
        weight = val[slot].reshape(-1, wide)
        hidden = jnp.maximum(
            jnp.dot(latent[slot], weight, preferred_element_type=jnp.float32), 0.0
        ).astype(jnp.bfloat16)
        vector = small[slot].astype(jnp.float32)[action_count : action_count + 1]
        value = jnp.sum(hidden.astype(jnp.float32) * vector, axis=-1, keepdims=True)
        model = total[slot] + discount**unroll * value[half:]
        lane = lax.broadcasted_iota(jnp.int32, (half, 2), 1)
        out_ref[slot] = jnp.where(lane == 0, value[:half], model)
    for copy in copies.made:
        copy.wait_send()


def copies_needed(groups, shards):
    chips = shards // CORES
    levels = 1 + groups // 2
    return 4 * groups + (2 * levels + 1) * chips + 3 * levels


def on_device(
    observations,
    rewards,
    actions,
    lengths,
    nsteps,
    prio_index,
    assignment,
    rep_weight,
    dyn_in,
    dyn_out,
    value_hidden,
    action_table,
    value_out,
    reward_out,
):
    groups = lax.axis_size("replica")
    batch, steps, width = observations.shape
    unroll = actions.shape[1] - steps
    picks = prio_index.shape[1]
    shards = lax.axis_size("shard")
    chips = shards // CORES
    me = lax.axis_index("replica")
    action_count = action_table.shape[1]
    hidden = rep_weight.shape[-1]
    small = jnp.concatenate([action_table[0], value_out, reward_out], axis=0)
    small = jnp.pad(small, ((0, -small.shape[0] % 32), (0, 0)))
    dyn = jnp.concatenate([dyn_in[0], dyn_out[0]], axis=0)

    owner = assignment[:, 0]
    ahead = (owner - me + groups) % groups
    slot_of = jnp.where(2 * ahead < groups, 2 * ahead, 2 * (groups - ahead) - 1)
    spot = slot_of * MOSTG + ranks_within(owner, groups)
    slots = groups * MOSTG
    match = spot[None, :] == jnp.arange(slots, dtype=jnp.int32)[:, None]
    source = jnp.sum(
        jnp.where(match, jnp.arange(batch, dtype=jnp.int32)[None, :], 0), axis=1
    )
    reach = prio_index + nsteps[:, None]
    alive = reach < lengths[:, None]
    reach = jnp.minimum(reach, steps - 1)
    base = jnp.arange(batch, dtype=jnp.int32)[:, None] * steps
    rows = jnp.concatenate([base + prio_index, base + reach], axis=1)
    moves = jnp.concatenate(
        [jnp.take_along_axis(actions, reach + depth, axis=1) for depth in range(unroll)], axis=1
    )
    packed = jnp.take(jnp.concatenate([rows, moves], axis=1), source, axis=0)
    packed = packed.reshape(groups, MOSTG, (2 + unroll), picks).transpose(0, 2, 1, 3)
    packed = packed.reshape(groups, 2 + unroll, MOSTG * picks)
    lines = packed[:, :2].reshape(groups, 2 * MOSTG * picks, 1)
    turns = packed[:, 2:].transpose(1, 0, 2)[..., None]
    rows = 2 * MOSTG * picks
    needed = copies_needed(groups, shards)

    def held(weight):
        return pltpu.VMEM((groups, chips, CORES) + weight.shape, weight.dtype)

    answered = pl.pallas_call(
        functools.partial(network_kernel, groups, shards, unroll, action_count),
        out_shape=jax.ShapeDtypeStruct((groups, rows // 2, 2), jnp.float32),
        in_specs=[pl.BlockSpec(memory_space=pltpu.VMEM)] * 7,
        out_specs=pl.BlockSpec(memory_space=pltpu.VMEM),
        scratch_shapes=[
            held(rep_weight[0]),
            held(dyn),
            held(value_hidden[0]),
            pltpu.VMEM((groups,) + small.shape, small.dtype),
            pltpu.VMEM((groups, rows, hidden), jnp.bfloat16),
            pltpu.VMEM((groups, rows, width), jnp.bfloat16),
            pltpu.VMEM((groups, rows // 2, 1), jnp.float32),
            pltpu.SemaphoreType.DMA((needed,)),
            pltpu.SemaphoreType.DMA((needed,)),
            pltpu.SemaphoreType.DMA((4,)),
        ],
        compiler_params=pltpu.CompilerParams(
            collective_id=0, has_side_effects=True, vmem_limit_bytes=56 * 1024 * 1024
        ),
    )(
        observations.reshape(batch * steps, width),
        lines,
        turns,
        rep_weight[0],
        dyn,
        value_hidden[0],
        small,
    )
    answered = answered.reshape(slots, picks * 2)
    back = jnp.take(answered, spot, axis=0).reshape(batch, picks, 2)
    bonus = discount ** nsteps.astype(jnp.float32)
    target = reward_part(rewards, lengths, nsteps, prio_index) + jnp.where(
        alive, bonus[:, None] * back[:, :, 1], 0.0
    )
    return jnp.abs(target - back[:, :, 0])


def solution(mesh):
    placed = (
        P(("replica", "shard"), None, None),
        P(("replica", "shard"), None),
        P(("replica", "shard"), None),
        P(("replica", "shard")),
        P(("replica", "shard")),
        P(("replica", "shard"), None),
        P(("replica", "shard"), None),
        P("replica", "shard", None),
        P("replica", "shard", None),
        P("replica", "shard", None),
        P("replica", "shard", None),
        P("replica", None, None),
        P("replica", None),
        P("replica", None),
    )
    return jax.shard_map(
        on_device,
        mesh=mesh,
        in_specs=placed,
        out_specs=P(("replica", "shard"), None),
        check_vma=False,
    )
```

```python
import functools
import math

import jax
import jax.numpy as jnp
from jax import lax
from jax.experimental import pallas as pl
from jax.experimental.pallas import tpu as pltpu
from jax.sharding import PartitionSpec as P

MOSTG = 32
CORES = 2
MESH = pl.DeviceIdType.MESH


discount = 0.997
epsilon = 1e-06


def rms_scale(values):
    return values * lax.rsqrt(jnp.mean(values * values, axis=-1, keepdims=True) + epsilon)


def ranks_within(owner, groups):
    member = (owner[:, None] == jnp.arange(groups, dtype=jnp.int32)[None, :]).astype(jnp.int32)
    earlier = jnp.cumsum(member, axis=0) - member
    return jnp.sum(earlier * member, axis=1)


def reward_part(rewards, lengths, nsteps, picks):
    position = jnp.arange(rewards.shape[1], dtype=jnp.int32)
    offset = position[None, None, :] - picks[:, :, None]
    inside = (
        (offset >= 0)
        & (offset < nsteps[:, None, None])
        & (position[None, None, :] < lengths[:, None, None])
    )
    power = discount ** jnp.maximum(offset, 0).astype(jnp.float32)
    return jnp.sum(jnp.where(inside, power, 0.0) * rewards[:, None, :], axis=2)


def chip_cycle(chips):
    side = max(d for d in range(1, math.isqrt(chips) + 1) if chips % d == 0)
    wide = chips // side
    if side % 2 or wide < 2:
        return list(range(chips))
    order = [0]
    for row in range(side):
        columns = range(1, wide) if row % 2 == 0 else range(wide - 1, 0, -1)
        order += [row * wide + column for column in columns]
    return order + [row * wide for row in range(side - 1, 0, -1)]


def lookup(table, index):
    found = jnp.int32(table[0])
    for place in range(1, len(table)):
        found = jnp.where(index == place, jnp.int32(table[place]), found)
    return found


class Copies:
    def __init__(self, send, recv):
        self.send, self.recv, self.made = send, recv, []

    def start(self, source, target, device):
        k = len(self.made)
        copy = pltpu.make_async_remote_copy(
            src_ref=source,
            dst_ref=target,
            send_sem=self.send.at[k],
            recv_sem=self.recv.at[k],
            device_id=device,
            device_id_type=MESH,
        )
        copy.start()
        self.made.append(copy)
        return copy


def network_kernel(
    groups,
    shards,
    unroll,
    action_count,
    obs_hbm,
    key_ref,
    acts_ref,
    spot_ref,
    rep_ref,
    in_ref,
    back_ref,
    val_ref,
    small_ref,
    out_ref,
    obs_ref,
    moves_ref,
    rep,
    dyn,
    val,
    small,
    latent,
    frames,
    total,
    send,
    recv,
    local,
):
    chips = shards // CORES
    half_ring, half_line = chips // 2, groups // 2
    me = lax.axis_index("replica")
    mine = lax.axis_index("shard")
    chip, core = mine // CORES, mine % CORES
    order = chip_cycle(chips)
    place = lookup([order.index(k) for k in range(chips)], chip)

    def at(distance):
        return lookup(order, lax.rem(place + distance + chips, chips))

    after, before = at(1), at(-1)
    up = (lax.rem(me + 1, groups), mine)
    down = (lax.rem(me + groups - 1, groups), mine)
    right = (me, after * CORES + core)
    left = (me, before * CORES + core)
    sibling = (me, chip * CORES + (1 - core))

    barrier = pltpu.get_barrier_semaphore()
    for device in (up, down, right, left, sibling):
        pl.semaphore_signal(barrier, inc=1, device_id=device, device_id_type=MESH)
    pl.semaphore_wait(barrier, 5)

    copies = Copies(send, recv)
    wide = rep_ref.shape[-1]
    halves = (pl.ds(0, wide // 2), pl.ds(wide // 2, wide // 2))

    def levels():
        return [(0, 1)] + [(2 * d - 1, 2) for d in range(1, half_line)] + [(groups - 1, 1)]

    def line(buffer, own, view, distance):
        pair = []
        for way, device in ((0, up), (1, down)):
            if distance == 1:
                source = own
            else:
                source = view(buffer.at[2 * (distance - 1) - 1 + way])
            last = distance == half_line
            slot = groups - 1 if last else 2 * distance - 1 + way
            target = view(buffer.at[slot])
            if last:
                source = source.at[(slice(None),) * (len(source.shape) - 1) + (halves[way],)]
                target = target.at[(slice(None),) * (len(target.shape) - 1) + (halves[way],)]
            pair.append(copies.start(source, target, device))
        return pair

    def ring(buffer, own, level, distance):
        first, count = level
        pair = []
        for way, device in ((0, right), (1, left)):
            origin = at((1 - distance) if way == 0 else (distance - 1))
            target = buffer.at[pl.ds(first, count), origin, core]
            source = own if own is not None and distance == 1 else target
            if own is not None and distance == 1:
                target = buffer.at[first, origin, core]
            if distance == half_ring:
                source = source.at[(slice(None),) * (len(source.shape) - 1) + (halves[way],)]
                target = target.at[(slice(None),) * (len(target.shape) - 1) + (halves[way],)]
            pair.append(copies.start(source, target, device))
        return pair

    def arrived(pair):
        for copy in pair:
            copy.wait_recv()

    def finish_ring(buffer, level, pair):
        for distance in range(2, half_ring + 1):
            arrived(pair)
            pair = ring(buffer, None, level, distance)
        return pair

    def share(buffer, level):
        first, count = level
        piece = buffer.at[pl.ds(first, count), :, core]
        return copies.start(piece, piece, sibling)

    def block(ref):
        return ref.at[chip, core]

    def plane(ref):
        return ref.at[:, core]

    def whole(ref):
        return ref

    rows_in = dyn.shape[3] // 2
    mine_dyn = dyn.at[0, chip, core]
    own = [
        pltpu.make_async_copy(in_ref, mine_dyn.at[pl.ds(0, rows_in)], local.at[0]),
        pltpu.make_async_copy(back_ref, mine_dyn.at[pl.ds(rows_in, rows_in)], local.at[1]),
        pltpu.make_async_copy(rep_ref, rep.at[0, chip, core], local.at[2]),
        pltpu.make_async_copy(val_ref, val.at[0, chip, core], local.at[3]),
        pltpu.make_async_copy(small_ref, small.at[0], local.at[4]),
        pltpu.make_async_copy(obs_hbm, obs_ref, local.at[5]),
    ]

    near, far = levels()[0], levels()[1:]
    rep_line = line(rep, rep_ref, block, 1)
    rep_ring = ring(rep, rep_ref, near, 1)
    for copy in own:
        copy.start()
    small_line = line(small, small_ref, whole, 1)
    val_ring = ring(val, val_ref, near, 1)
    own[0].wait()
    own[1].wait()
    dyn_line = line(dyn, mine_dyn, block, 1)
    dyn_ring = ring(dyn, None, near, 1)
    for copy in own[2:]:
        copy.wait()

    kinds = key_ref.shape[0]
    most = frames.shape[1] // kinds
    picks = kinds // 2
    half = picks * most
    observed = obs_ref.shape[0]

    def pick(slot, carry):
        rank = slot * most + lax.broadcasted_iota(jnp.int32, (most, observed), 0)
        one_hot = jnp.concatenate(
            [
                jnp.where(key_ref[kind : kind + 1] == rank, 1.0, 0.0).astype(jnp.bfloat16)
                for kind in range(kinds)
            ],
            axis=0,
        )
        frames[slot] = jnp.dot(
            one_hot, obs_ref[...], preferred_element_type=jnp.float32
        ).astype(jnp.bfloat16)
        moves_ref[slot] = jnp.dot(
            one_hot[half:], acts_ref[...], preferred_element_type=jnp.float32
        )
        return carry

    lax.fori_loop(0, groups, pick, 0)

    rep_far, dyn_far = [], []
    for index, level in enumerate(far):
        distance = index + 1
        arrived(rep_line)
        if distance < half_line:
            rep_line = line(rep, None, block, distance + 1)
        rep_far.append(ring(rep, None, level, 1))
        if index == 0:
            rep_ring = finish_ring(rep, near, rep_ring)
            val_ring = finish_ring(val, near, val_ring)
        arrived(small_line)
        if distance < half_line:
            small_line = line(small, None, whole, distance + 1)
        arrived(dyn_line)
        if distance < half_line:
            dyn_line = line(dyn, None, block, distance + 1)
        if index == 0:
            arrived(val_ring)
            val_line = line(val, val.at[0, :, core], plane, 1)
            dyn_ring = finish_ring(dyn, near, dyn_ring)
        dyn_far.append(ring(dyn, None, level, 1))

    def represent(level):
        for slot in range(level[0], level[0] + level[1]):
            weight = rep[slot].reshape(-1, wide)
            raw = jnp.dot(frames[slot], weight, preferred_element_type=jnp.float32)
            latent[slot] = rms_scale(raw).astype(jnp.bfloat16)

    def unrolled(level):
        slots = range(level[0], level[0] + level[1])
        lane = lax.broadcasted_iota(jnp.int32, (half, moves_ref.shape[-1]), 1)

        def advance(depth, carry):
            scale, totals = carry
            grown = []
            for slot, so_far in zip(slots, totals):
                first = dyn[slot, :, :, :rows_in].reshape(-1, wide)
                second = dyn[slot, :, :, rows_in:].reshape(-1, wide)
                table = small[slot]
                move = jnp.sum(
                    jnp.where(lane == depth, moves_ref[slot], 0.0), axis=-1, keepdims=True
                ).astype(jnp.int32)
                one_hot = jnp.where(
                    move == lax.broadcasted_iota(jnp.int32, (half, table.shape[0]), 1), 1.0, 0.0
                ).astype(jnp.bfloat16)
                state = latent[slot, half:]
                inner = jnp.maximum(
                    jnp.dot(state, first, preferred_element_type=jnp.float32)
                    + jnp.dot(one_hot, table, preferred_element_type=jnp.float32),
                    0.0,
                ).astype(jnp.bfloat16)
                update = jnp.dot(inner, second, preferred_element_type=jnp.float32)
                state = rms_scale(state.astype(jnp.float32) + update).astype(jnp.bfloat16)
                latent[slot, half:] = state
                vector = table.astype(jnp.float32)[action_count + 1 : action_count + 2]
                guess = jnp.sum(state.astype(jnp.float32) * vector, axis=-1, keepdims=True)
                grown.append(so_far + scale * guess)
            return scale * discount, tuple(grown)

        zeros = tuple(jnp.zeros((half, 1), jnp.float32) for _ in slots)
        _, totals = lax.fori_loop(0, unroll, advance, (jnp.float32(1.0), zeros))
        for slot, so_far in zip(slots, totals):
            total[slot] = so_far

    for index, level in enumerate(far):
        rep_far[index] = finish_ring(rep, level, rep_far[index])
    arrived(rep_ring)
    rep_shared = [share(rep, near)]
    dyn_far[0] = finish_ring(dyn, far[0], dyn_far[0])
    arrived(rep_far[0])
    rep_shared.append(share(rep, far[0]))
    arrived(dyn_ring)
    dyn_shared = [share(dyn, near)]
    val_shared = [share(val, near)]
    arrived(rep_shared[:1])
    represent(near)
    for index, level in list(enumerate(far))[1:]:
        dyn_far[index] = finish_ring(dyn, level, dyn_far[index])
        arrived(rep_far[index])
        rep_shared.append(share(rep, level))
    for distance in range(2, half_line + 1):
        arrived(val_line)
        val_line = line(val, None, plane, distance)
        val_shared.append(share(val, far[distance - 2]))
    for index, level in enumerate(far[:-1]):
        arrived(rep_shared[index + 1 : index + 2])
        represent(level)
    arrived(dyn_shared[:1])
    unrolled(near)
    for index, level in enumerate(far):
        arrived(dyn_far[index])
        dyn_shared.append(share(dyn, level))
    arrived(rep_shared[-1:])
    represent(far[-1])
    for index, level in enumerate(far[:-1]):
        arrived(dyn_shared[index + 1 : index + 2])
        unrolled(level)
    arrived(val_line)
    val_shared.append(share(val, far[-1]))
    arrived(dyn_shared[-1:])
    unrolled(far[-1])
    arrived(val_shared)

    answers = [0.0] * kinds
    for slot in range(groups):
        weight = val[slot].reshape(-1, wide)
        hidden = jnp.maximum(
            jnp.dot(latent[slot], weight, preferred_element_type=jnp.float32), 0.0
        ).astype(jnp.bfloat16)
        vector = small[slot].astype(jnp.float32)[action_count : action_count + 1]
        value = jnp.sum(hidden.astype(jnp.float32) * vector, axis=-1, keepdims=True)
        model = total[slot] + discount**unroll * value[half:]
        rank = slot * most + lax.broadcasted_iota(jnp.int32, (most, spot_ref.shape[1]), 0)
        here = spot_ref[...] == rank
        for kind in range(kinds):
            source = value if kind < picks else model
            part = source[kind % picks * most : (kind % picks + 1) * most]
            answers[kind] += jnp.sum(jnp.where(here, part, 0.0), axis=0, keepdims=True)
    out_ref[...] = jnp.concatenate(answers, axis=0)
    for copy in copies.made:
        copy.wait_send()


def copies_needed(groups, shards):
    chips = shards // CORES
    levels = 1 + groups // 2
    return 4 * groups + (2 * levels + 1) * chips + 3 * levels


def on_device(
    observations,
    rewards,
    actions,
    lengths,
    nsteps,
    prio_index,
    assignment,
    rep_weight,
    dyn_in,
    dyn_out,
    value_hidden,
    action_table,
    value_out,
    reward_out,
):
    groups = lax.axis_size("replica")
    batch, steps, width = observations.shape
    unroll = actions.shape[1] - steps
    picks = prio_index.shape[1]
    shards = lax.axis_size("shard")
    chips = shards // CORES
    me = lax.axis_index("replica")
    action_count = action_table.shape[1]
    hidden = rep_weight.shape[-1]
    small = jnp.concatenate([action_table[0], value_out, reward_out], axis=0)
    small = jnp.pad(small, ((0, -small.shape[0] % 32), (0, 0)))

    owner = assignment[:, 0]
    ahead = (owner - me + groups) % groups
    slot_of = jnp.where(2 * ahead < groups, 2 * ahead, 2 * (groups - ahead) - 1)
    spot = slot_of * MOSTG + ranks_within(owner, groups)
    reach = prio_index + nsteps[:, None]
    alive = reach < lengths[:, None]
    reach = jnp.minimum(reach, steps - 1)
    wanted = jnp.concatenate([prio_index, reach], axis=1).T
    step = jnp.arange(steps, dtype=jnp.int32)
    key = jnp.where(wanted[:, :, None] == step[None, None, :], spot[None, :, None], -1)
    key = key.reshape(2 * picks, batch * steps)
    acts = jnp.stack([actions[:, depth : depth + steps] for depth in range(unroll)], axis=2)
    acts = acts.astype(jnp.bfloat16).reshape(batch * steps, unroll)
    acts = jnp.pad(acts, ((0, 0), (0, -unroll % 128)))
    rows = 2 * MOSTG * picks
    needed = copies_needed(groups, shards)

    def held(count):
        return pltpu.VMEM((groups, chips, CORES, count, hidden), jnp.bfloat16)

    answered = pl.pallas_call(
        functools.partial(network_kernel, groups, shards, unroll, action_count),
        out_shape=jax.ShapeDtypeStruct((2 * picks, batch), jnp.float32),
        in_specs=[pl.BlockSpec(memory_space=pl.ANY)]
        + [pl.BlockSpec(memory_space=pltpu.VMEM)] * 8,
        out_specs=pl.BlockSpec(memory_space=pltpu.VMEM),
        scratch_shapes=[
            pltpu.VMEM((batch * steps, width), jnp.bfloat16),
            pltpu.VMEM((groups, rows // 2, acts.shape[1]), jnp.float32),
            held(rep_weight.shape[1]),
            held(dyn_in.shape[1] + dyn_out.shape[1]),
            held(value_hidden.shape[1]),
            pltpu.VMEM((groups,) + small.shape, small.dtype),
            pltpu.VMEM((groups, rows, hidden), jnp.bfloat16),
            pltpu.VMEM((groups, rows, width), jnp.bfloat16),
            pltpu.VMEM((groups, rows // 2, 1), jnp.float32),
            pltpu.SemaphoreType.DMA((needed,)),
            pltpu.SemaphoreType.DMA((needed,)),
            pltpu.SemaphoreType.DMA((6,)),
        ],
        compiler_params=pltpu.CompilerParams(
            collective_id=0, has_side_effects=True, vmem_limit_bytes=56 * 1024 * 1024
        ),
    )(
        observations.reshape(batch * steps, width),
        key,
        acts,
        spot[None, :],
        rep_weight[0],
        dyn_in[0],
        dyn_out[0],
        value_hidden[0],
        small,
    )
    root_value, model_return = answered[:picks].T, answered[picks:].T
    bonus = discount ** nsteps.astype(jnp.float32)
    target = reward_part(rewards, lengths, nsteps, prio_index) + jnp.where(
        alive, bonus[:, None] * model_return, 0.0
    )
    return jnp.abs(target - root_value)


def solution(mesh):
    placed = (
        P(("replica", "shard"), None, None),
        P(("replica", "shard"), None),
        P(("replica", "shard"), None),
        P(("replica", "shard")),
        P(("replica", "shard")),
        P(("replica", "shard"), None),
        P(("replica", "shard"), None),
        P("replica", "shard", None),
        P("replica", "shard", None),
        P("replica", "shard", None),
        P("replica", "shard", None),
        P("replica", None, None),
        P("replica", None),
        P("replica", None),
    )
    return jax.shard_map(
        on_device,
        mesh=mesh,
        in_specs=placed,
        out_specs=P(("replica", "shard"), None),
        check_vma=False,
    )
```

```python
import functools
import math

import jax
import jax.numpy as jnp
from jax import lax
from jax.experimental import pallas as pl
from jax.experimental.pallas import tpu as pltpu
from jax.sharding import PartitionSpec as P

MOSTG = 32
CORES = 2
MESH = pl.DeviceIdType.MESH


discount = 0.997
epsilon = 1e-06


def rms_scale(values):
    return values * lax.rsqrt(jnp.mean(values * values, axis=-1, keepdims=True) + epsilon)


def ranks_within(owner):
    place = jnp.arange(owner.shape[0], dtype=jnp.int32)
    earlier = (owner[None, :] == owner[:, None]) & (place[None, :] < place[:, None])
    return jnp.sum(earlier.astype(jnp.int32), axis=1)


def reward_part(rewards, lengths, nsteps, picks):
    position = jnp.arange(rewards.shape[1], dtype=jnp.int32)
    offset = position[None, None, :] - picks[:, :, None]
    inside = (
        (offset >= 0)
        & (offset < nsteps[:, None, None])
        & (position[None, None, :] < lengths[:, None, None])
    )
    power = discount ** jnp.maximum(offset, 0).astype(jnp.float32)
    return jnp.sum(jnp.where(inside, power, 0.0) * rewards[:, None, :], axis=2)


def chip_cycle(chips):
    side = max(d for d in range(1, math.isqrt(chips) + 1) if chips % d == 0)
    wide = chips // side
    if side % 2 or wide < 2:
        return list(range(chips))
    order = [0]
    for row in range(side):
        columns = range(1, wide) if row % 2 == 0 else range(wide - 1, 0, -1)
        order += [row * wide + column for column in columns]
    return order + [row * wide for row in range(side - 1, 0, -1)]


def lookup(table, index):
    found = jnp.int32(table[0])
    for place in range(1, len(table)):
        found = jnp.where(index == place, jnp.int32(table[place]), found)
    return found


class Copies:
    def __init__(self, send, recv):
        self.send, self.recv, self.made = send, recv, []

    def start(self, source, target, device):
        k = len(self.made)
        copy = pltpu.make_async_remote_copy(
            src_ref=source,
            dst_ref=target,
            send_sem=self.send.at[k],
            recv_sem=self.recv.at[k],
            device_id=device,
            device_id_type=MESH,
        )
        copy.start()
        self.made.append(copy)
        return copy


def network_kernel(
    groups,
    shards,
    unroll,
    action_count,
    obs_hbm,
    key_ref,
    acts_ref,
    spot_ref,
    rep_ref,
    in_ref,
    back_ref,
    val_ref,
    small_ref,
    out_ref,
    obs_ref,
    moves_ref,
    rep,
    dyn,
    val,
    small,
    latent,
    frames,
    total,
    send,
    recv,
    local,
):
    chips = shards // CORES
    half_ring, half_line = chips // 2, groups // 2
    me = lax.axis_index("replica")
    mine = lax.axis_index("shard")
    chip, core = mine // CORES, mine % CORES
    order = chip_cycle(chips)
    place = lookup([order.index(k) for k in range(chips)], chip)

    def at(distance):
        return lookup(order, lax.rem(place + distance + chips, chips))

    after, before = at(1), at(-1)
    up = (lax.rem(me + 1, groups), mine)
    down = (lax.rem(me + groups - 1, groups), mine)
    right = (me, after * CORES + core)
    left = (me, before * CORES + core)
    sibling = (me, chip * CORES + (1 - core))

    barrier = pltpu.get_barrier_semaphore()
    for device in (up, down, right, left, sibling):
        pl.semaphore_signal(barrier, inc=1, device_id=device, device_id_type=MESH)
    pl.semaphore_wait(barrier, 5)

    copies = Copies(send, recv)
    wide = rep_ref.shape[-1]
    halves = (pl.ds(0, wide // 2), pl.ds(wide // 2, wide // 2))

    def levels():
        return [(0, 1)] + [(2 * d - 1, 2) for d in range(1, half_line)] + [(groups - 1, 1)]

    def line(buffer, own, view, distance):
        pair = []
        for way, device in ((0, up), (1, down)):
            if distance == 1:
                source = own
            else:
                source = view(buffer.at[2 * (distance - 1) - 1 + way])
            last = distance == half_line
            slot = groups - 1 if last else 2 * distance - 1 + way
            target = view(buffer.at[slot])
            if last:
                source = source.at[(slice(None),) * (len(source.shape) - 1) + (halves[way],)]
                target = target.at[(slice(None),) * (len(target.shape) - 1) + (halves[way],)]
            pair.append(copies.start(source, target, device))
        return pair

    def ring(buffer, own, level, distance):
        first, count = level
        pair = []
        for way, device in ((0, right), (1, left)):
            origin = at((1 - distance) if way == 0 else (distance - 1))
            target = buffer.at[pl.ds(first, count), origin, core]
            source = own if own is not None and distance == 1 else target
            if own is not None and distance == 1:
                target = buffer.at[first, origin, core]
            if distance == half_ring:
                source = source.at[(slice(None),) * (len(source.shape) - 1) + (halves[way],)]
                target = target.at[(slice(None),) * (len(target.shape) - 1) + (halves[way],)]
            pair.append(copies.start(source, target, device))
        return pair

    def arrived(pair):
        for copy in pair:
            copy.wait_recv()

    def finish_ring(buffer, level, pair):
        for distance in range(2, half_ring + 1):
            arrived(pair)
            pair = ring(buffer, None, level, distance)
        return pair

    def share(buffer, level):
        first, count = level
        piece = buffer.at[pl.ds(first, count), :, core]
        return copies.start(piece, piece, sibling)

    def block(ref):
        return ref.at[chip, core]

    def plane(ref):
        return ref.at[:, core]

    def whole(ref):
        return ref

    rows_in = dyn.shape[3] // 2
    mine_dyn = dyn.at[0, chip, core]
    own = [
        pltpu.make_async_copy(in_ref, mine_dyn.at[pl.ds(0, rows_in)], local.at[0]),
        pltpu.make_async_copy(back_ref, mine_dyn.at[pl.ds(rows_in, rows_in)], local.at[1]),
        pltpu.make_async_copy(rep_ref, rep.at[0, chip, core], local.at[2]),
        pltpu.make_async_copy(val_ref, val.at[0, chip, core], local.at[3]),
        pltpu.make_async_copy(small_ref, small.at[0], local.at[4]),
        pltpu.make_async_copy(obs_hbm, obs_ref, local.at[5]),
    ]

    near, far = levels()[0], levels()[1:]
    rep_line = line(rep, rep_ref, block, 1)
    rep_ring = ring(rep, rep_ref, near, 1)
    for copy in own:
        copy.start()
    small_line = line(small, small_ref, whole, 1)
    val_ring = ring(val, val_ref, near, 1)
    own[0].wait()
    own[1].wait()
    dyn_line = line(dyn, mine_dyn, block, 1)
    dyn_ring = ring(dyn, None, near, 1)
    for copy in own[2:]:
        copy.wait()

    kinds = key_ref.shape[0]
    most = frames.shape[1] // kinds
    picks = kinds // 2
    half = picks * most
    observed = obs_ref.shape[0]

    def pick(slot, carry):
        rank = slot * most + lax.broadcasted_iota(jnp.int32, (most, observed), 0)
        one_hot = jnp.concatenate(
            [
                jnp.where(key_ref[kind : kind + 1] == rank, 1.0, 0.0).astype(jnp.bfloat16)
                for kind in range(kinds)
            ],
            axis=0,
        )
        frames[slot] = jnp.dot(
            one_hot, obs_ref[...], preferred_element_type=jnp.float32
        ).astype(jnp.bfloat16)
        moves_ref[slot] = jnp.dot(
            one_hot[half:], acts_ref[...], preferred_element_type=jnp.float32
        )
        return carry

    lax.fori_loop(0, groups, pick, 0)

    rep_far, dyn_far = [], []
    for index, level in enumerate(far):
        distance = index + 1
        arrived(rep_line)
        if distance < half_line:
            rep_line = line(rep, None, block, distance + 1)
        rep_far.append(ring(rep, None, level, 1))
        if index == 0:
            rep_ring = finish_ring(rep, near, rep_ring)
            val_ring = finish_ring(val, near, val_ring)
        arrived(small_line)
        if distance < half_line:
            small_line = line(small, None, whole, distance + 1)
        arrived(dyn_line)
        if distance < half_line:
            dyn_line = line(dyn, None, block, distance + 1)
        if index == 0:
            arrived(val_ring)
            val_line = line(val, val.at[0, :, core], plane, 1)
            dyn_ring = finish_ring(dyn, near, dyn_ring)
        dyn_far.append(ring(dyn, None, level, 1))

    def represent(level):
        for slot in range(level[0], level[0] + level[1]):
            weight = rep[slot].reshape(-1, wide)
            raw = jnp.dot(frames[slot], weight, preferred_element_type=jnp.float32)
            latent[slot] = rms_scale(raw).astype(jnp.bfloat16)

    def unrolled(level):
        slots = range(level[0], level[0] + level[1])
        lane = lax.broadcasted_iota(jnp.int32, (half, moves_ref.shape[-1]), 1)

        def advance(depth, carry):
            scale, totals = carry
            grown = []
            for slot, so_far in zip(slots, totals):
                first = dyn[slot, :, :, :rows_in].reshape(-1, wide)
                second = dyn[slot, :, :, rows_in:].reshape(-1, wide)
                table = small[slot]
                move = jnp.sum(
                    jnp.where(lane == depth, moves_ref[slot], 0.0), axis=-1, keepdims=True
                ).astype(jnp.int32)
                one_hot = jnp.where(
                    move == lax.broadcasted_iota(jnp.int32, (half, table.shape[0]), 1), 1.0, 0.0
                ).astype(jnp.bfloat16)
                state = latent[slot, half:]
                inner = jnp.maximum(
                    jnp.dot(state, first, preferred_element_type=jnp.float32)
                    + jnp.dot(one_hot, table, preferred_element_type=jnp.float32),
                    0.0,
                ).astype(jnp.bfloat16)
                update = jnp.dot(inner, second, preferred_element_type=jnp.float32)
                state = rms_scale(state.astype(jnp.float32) + update).astype(jnp.bfloat16)
                latent[slot, half:] = state
                vector = table.astype(jnp.float32)[action_count + 1 : action_count + 2]
                guess = jnp.sum(state.astype(jnp.float32) * vector, axis=-1, keepdims=True)
                grown.append(so_far + scale * guess)
            return scale * discount, tuple(grown)

        zeros = tuple(jnp.zeros((half, 1), jnp.float32) for _ in slots)
        _, totals = lax.fori_loop(0, unroll, advance, (jnp.float32(1.0), zeros))
        for slot, so_far in zip(slots, totals):
            total[slot] = so_far

    for index, level in enumerate(far):
        rep_far[index] = finish_ring(rep, level, rep_far[index])
    arrived(rep_ring)
    rep_shared = [share(rep, near)]
    dyn_far[0] = finish_ring(dyn, far[0], dyn_far[0])
    arrived(rep_far[0])
    rep_shared.append(share(rep, far[0]))
    arrived(dyn_ring)
    dyn_shared = [share(dyn, near)]
    val_shared = [share(val, near)]
    arrived(rep_shared[:1])
    represent(near)
    for index, level in list(enumerate(far))[1:]:
        dyn_far[index] = finish_ring(dyn, level, dyn_far[index])
        arrived(rep_far[index])
        rep_shared.append(share(rep, level))
    for index, level in enumerate(far[:-1]):
        arrived(rep_shared[index + 1 : index + 2])
        represent(level)
    arrived(dyn_shared[:1])
    unrolled(near)
    for distance in range(2, half_line + 1):
        arrived(val_line)
        val_line = line(val, None, plane, distance)
        val_shared.append(share(val, far[distance - 2]))
    for index, level in enumerate(far):
        arrived(dyn_far[index])
        dyn_shared.append(share(dyn, level))
    arrived(rep_shared[-1:])
    represent(far[-1])
    arrived(dyn_shared[1:])
    unrolled((1, groups - 1))
    arrived(val_line)
    val_shared.append(share(val, far[-1]))
    arrived(val_shared)

    answers = [0.0] * kinds
    for slot in range(groups):
        weight = val[slot].reshape(-1, wide)
        hidden = jnp.maximum(
            jnp.dot(latent[slot], weight, preferred_element_type=jnp.float32), 0.0
        ).astype(jnp.bfloat16)
        vector = small[slot].astype(jnp.float32)[action_count : action_count + 1]
        value = jnp.sum(hidden.astype(jnp.float32) * vector, axis=-1, keepdims=True)
        model = total[slot] + discount**unroll * value[half:]
        rank = slot * most + lax.broadcasted_iota(jnp.int32, (most, spot_ref.shape[1]), 0)
        here = spot_ref[...] == rank
        for kind in range(kinds):
            source = value if kind < picks else model
            part = source[kind % picks * most : (kind % picks + 1) * most]
            answers[kind] += jnp.sum(jnp.where(here, part, 0.0), axis=0, keepdims=True)
    out_ref[...] = jnp.concatenate(answers, axis=0)
    for copy in copies.made:
        copy.wait_send()


def copies_needed(groups, shards):
    chips = shards // CORES
    levels = 1 + groups // 2
    return 4 * groups + (2 * levels + 1) * chips + 3 * levels


def on_device(
    observations,
    rewards,
    actions,
    lengths,
    nsteps,
    prio_index,
    assignment,
    rep_weight,
    dyn_in,
    dyn_out,
    value_hidden,
    action_table,
    value_out,
    reward_out,
):
    groups = lax.axis_size("replica")
    batch, steps, width = observations.shape
    unroll = actions.shape[1] - steps
    picks = prio_index.shape[1]
    shards = lax.axis_size("shard")
    chips = shards // CORES
    me = lax.axis_index("replica")
    action_count = action_table.shape[1]
    hidden = rep_weight.shape[-1]
    small = jnp.concatenate([action_table[0], value_out, reward_out], axis=0)
    small = jnp.pad(small, ((0, -small.shape[0] % 32), (0, 0)))

    owner = assignment[:, 0]
    ahead = (owner - me + groups) % groups
    slot_of = jnp.where(2 * ahead < groups, 2 * ahead, 2 * (groups - ahead) - 1)
    spot = slot_of * MOSTG + ranks_within(owner)
    reach = prio_index + nsteps[:, None]
    alive = reach < lengths[:, None]
    reach = jnp.minimum(reach, steps - 1)
    wanted = jnp.concatenate([prio_index, reach], axis=1).T
    step = jnp.arange(steps, dtype=jnp.int32)
    key = jnp.where(wanted[:, :, None] == step[None, None, :], spot[None, :, None], -1)
    key = key.reshape(2 * picks, batch * steps)
    acts = jnp.stack([actions[:, depth : depth + steps] for depth in range(unroll)], axis=2)
    acts = acts.astype(jnp.bfloat16).reshape(batch * steps, unroll)
    acts = jnp.pad(acts, ((0, 0), (0, -unroll % 128)))
    rows = 2 * MOSTG * picks
    needed = copies_needed(groups, shards)

    def held(count):
        return pltpu.VMEM((groups, chips, CORES, count, hidden), jnp.bfloat16)

    answered = pl.pallas_call(
        functools.partial(network_kernel, groups, shards, unroll, action_count),
        out_shape=jax.ShapeDtypeStruct((2 * picks, batch), jnp.float32),
        in_specs=[pl.BlockSpec(memory_space=pl.ANY)]
        + [pl.BlockSpec(memory_space=pltpu.VMEM)] * 8,
        out_specs=pl.BlockSpec(memory_space=pltpu.VMEM),
        scratch_shapes=[
            pltpu.VMEM((batch * steps, width), jnp.bfloat16),
            pltpu.VMEM((groups, rows // 2, acts.shape[1]), jnp.float32),
            held(rep_weight.shape[1]),
            held(dyn_in.shape[1] + dyn_out.shape[1]),
            held(value_hidden.shape[1]),
            pltpu.VMEM((groups,) + small.shape, small.dtype),
            pltpu.VMEM((groups, rows, hidden), jnp.bfloat16),
            pltpu.VMEM((groups, rows, width), jnp.bfloat16),
            pltpu.VMEM((groups, rows // 2, 1), jnp.float32),
            pltpu.SemaphoreType.DMA((needed,)),
            pltpu.SemaphoreType.DMA((needed,)),
            pltpu.SemaphoreType.DMA((6,)),
        ],
        compiler_params=pltpu.CompilerParams(
            collective_id=0, has_side_effects=True, vmem_limit_bytes=56 * 1024 * 1024
        ),
    )(
        observations.reshape(batch * steps, width),
        key,
        acts,
        spot[None, :],
        rep_weight[0],
        dyn_in[0],
        dyn_out[0],
        value_hidden[0],
        small,
    )
    root_value, model_return = answered[:picks].T, answered[picks:].T
    bonus = discount ** nsteps.astype(jnp.float32)
    target = reward_part(rewards, lengths, nsteps, prio_index) + jnp.where(
        alive, bonus[:, None] * model_return, 0.0
    )
    return jnp.abs(target - root_value)


def solution(mesh):
    placed = (
        P(("replica", "shard"), None, None),
        P(("replica", "shard"), None),
        P(("replica", "shard"), None),
        P(("replica", "shard")),
        P(("replica", "shard")),
        P(("replica", "shard"), None),
        P(("replica", "shard"), None),
        P("replica", "shard", None),
        P("replica", "shard", None),
        P("replica", "shard", None),
        P("replica", "shard", None),
        P("replica", None, None),
        P("replica", None),
        P("replica", None),
    )
    return jax.shard_map(
        on_device,
        mesh=mesh,
        in_specs=placed,
        out_specs=P(("replica", "shard"), None),
        check_vma=False,
    )
```
